256 devices in a mesh: var: 32 (over y, z_hi, core), smp: 8 (over z_lo, x).
Axes of the slice: x: 4, y: 4, z: 8 (z_hi: 4, z_lo: 2; z = z_hi * 2 + z_lo), core: 2. Of those that a mesh axis runs over, the one named last changes fastest.
Arguments:
- genotype: bfloat16 [65536, 16384], P('var', 'smp'), may hold values from 0 to 2
- labels: int32 [65536], P('var'), may hold values from 0 to 7, as said below
- probes: bfloat16 [20, 16384], P(None, 'smp'), may hold values from -6 to 6
- phenotype: bfloat16 [16384], P('smp'), may hold values from -6 to 6
Outputs:
- moments: float32 [8, 21, 8, 2048], P(None, None, 'smp', 'var')
The draws below stay inside these ranges and needn't reach their ends.
Inputs may be any that keep to these rules, and one draw needn't show every extreme that they name: Within each aligned block of 2048 variants the labels never fall, and every one of the 8 components appears in every block.
All inputs are finite; a program needn't handle non-finite values.
Results may differ from the reference program's by a relative error of at most 0.0039.
Values sent between devices are 32-bit elements; how exact they have to be, the bound alone decides.
No kernel may reach another device: no remote copies, remote signals or barrier semaphores. Data moves between devices by JAX's collectives and lax.ppermute only.
A program may use at most 64 MiB of HBM per device.

```python
import math
import jax
import jax.numpy as jnp
from jax import lax

VDEV = 2048
NB = 20
K = 8
NV = 21
M = 65536
R = 2048
Q = 8
N = 16384


def draw_genotype(key, part):
    first, second, third = jax.random.split(jax.random.fold_in(key, 11), 3)
    base = jax.random.uniform(first, (M, 1), jnp.float32, 0.0, 0.7)
    width = jnp.exp(jax.random.uniform(second, (M, 1), jnp.float32, math.log(0.08), math.log(0.9)))
    noise = jax.random.uniform(third, (M, N), jnp.float32)
    return (base + width * noise).astype(jnp.bfloat16)


def draw_labels(key, part):
    first, second = jax.random.split(jax.random.fold_in(key, 23), 2)
    blocks = M // VDEV
    span = max(blocks - 1, 1)
    place = jnp.arange(blocks, dtype=jnp.int32)[:, None]
    comp = jnp.arange(8, dtype=jnp.int32)[None, :]
    rising = span + 3 * place
    falling = 4 * span - 3 * place
    base_weight = jnp.where(comp % 2 == 0, rising, falling)
    jitter = jax.random.randint(second, (blocks, 8), 0, span // 2 + 1)
    cumulative = jnp.cumsum(base_weight + jitter, axis=1).astype(jnp.int32)
    whole = cumulative[:, 7:8]
    raw = jax.random.randint(first, (blocks, VDEV), 0, whole)
    level = jnp.sum((raw[:, :, None] >= cumulative[:, None, :]).astype(jnp.int32), axis=2)
    position = jnp.arange(VDEV, dtype=jnp.int32)[None, :]
    level = jnp.where(position < 8, position % 8, level)
    return jnp.sort(level, axis=1).reshape(M).astype(jnp.int32)


def level_of(rng, extent, shards, smallest, largest):
    factor_of, own = 1.0, jax.random.fold_in(rng, 6)
    for dim, shards_of in shards:
        steps = jnp.exp(jax.random.uniform(jax.random.fold_in(own, dim), (shards_of,), jnp.float32, smallest / len(shards), largest / len(shards)))
        factor_of = factor_of * jnp.repeat(steps, extent[dim] // shards_of).reshape([-1 if axis == dim else 1 for axis in range(len(extent))])
    return factor_of


def centred(rng, dims, scale, limit, cuts=(), held_as=jnp.bfloat16):
    gain = level_of(rng, dims, cuts, -0.22, 0.18) if cuts else 1.0
    values = jax.random.normal(rng, dims, jnp.float32) * scale * gain
    return jnp.minimum(jnp.maximum(values, -limit), limit).astype(held_as)


def setup_inputs(seed: int = 0) -> dict:
    keys = jax.random.split(jax.random.key(seed), 5)
    genotype = draw_genotype(jax.random.fold_in(keys[4], 71), 0)
    labels = draw_labels(jax.random.fold_in(keys[4], 71), 0)
    probes = centred(keys[2], (NB, N), 1.0, 6.0, ((1, 8),))
    phenotype = centred(keys[3], (N,), 1.0, 6.0, ((0, 8),))
    return {"genotype": genotype, "labels": labels, "probes": probes, "phenotype": phenotype}


EPS = 1e-06

def reference(genotype, labels, probes, phenotype):
    vectors = jnp.concatenate([probes, phenotype[None, :]], axis=0)
    member = (labels[None, :] == jnp.arange(K, dtype=jnp.int32)[:, None]).astype(jnp.float32)
    counts = lax.optimization_barrier(jnp.sum(member, axis=1))
    blocks = M // VDEV

    def step(carry, index):
        start = (index * VDEV).astype(jnp.int32)
        dosage = lax.dynamic_slice_in_dim(genotype, start, VDEV, 0).astype(jnp.float32)
        mean = lax.optimization_barrier(jnp.sum(dosage, axis=1)) / N
        centered = dosage - mean[:, None]
        spread = lax.optimization_barrier(jnp.sum(centered * centered, axis=1)) / N
        scaled = (centered * lax.rsqrt(spread + EPS)[:, None]).astype(jnp.bfloat16)
        projected = lax.dot_general(vectors, scaled, (((1,), (1,)), ((), ())), preferred_element_type=jnp.float32)
        local_member = lax.dynamic_slice_in_dim(member, start, VDEV, 1)
        weights = (projected[None, :, :] * local_member[:, None, :] / counts[:, None, None]).astype(jnp.bfloat16)
        weights = weights.reshape(K * NV, VDEV)
        return (carry + jnp.dot(weights, scaled, preferred_element_type=jnp.float32), None)
    start_value = jnp.zeros((K * NV, N), jnp.float32)
    total, unused = lax.scan(step, start_value, jnp.arange(blocks, dtype=jnp.int32))
    return total.reshape(K, NV, Q, R)
```

```python
import jax
import jax.numpy as jnp
from jax import lax
from jax.experimental import pallas as pl
from jax.experimental.pallas import tpu as pltpu
from jax.sharding import PartitionSpec as P

K = 8
NV = 21
EPS = 1e-06
N = 16384

MEAN, SQUARES, VSUM = 21, 22, 23
ROWS = 24
STEP = 256


def shifted(array, axis, perm):
    return lax.ppermute(array, axis, perm)


ZLO_SWAP = [(i, i ^ 4) for i in range(8)]
X_UP = [(i, (i & 4) | ((i + 1) & 3)) for i in range(8)]
X_DOWN = [(i, (i & 4) | ((i - 1) & 3)) for i in range(8)]
CORE_SWAP = [(i, i ^ 1) for i in range(32)]
Y_UP = [(i, (i + 8) % 32) for i in range(32)]
Y_ACROSS = [(i, (i + 16) % 32) for i in range(32)]
Y_DOWN = [(i, (i - 8) % 32) for i in range(32)]
Z_UP = [(i, (i & 25) | ((i + 2) & 6)) for i in range(32)]
Z_ACROSS = [(i, i ^ 4) for i in range(32)]
Z_DOWN = [(i, (i & 25) | ((i - 2) & 6)) for i in range(32)]


def stats_kernel(probes, phenotype, genotype, out, vec, vsum):
    samples = genotype.shape[1]
    step = pl.program_id(0)

    @pl.when(step == 0)
    def _():
        row = lax.broadcasted_iota(jnp.int32, (32, samples), 0)
        low = jnp.concatenate([probes[...].astype(jnp.float32), jnp.zeros((12, samples), jnp.float32)], axis=0)
        low = jnp.where(row == NV - 1, phenotype[...], jnp.where(row == MEAN, 1.0, low))
        full = jnp.concatenate([low, jnp.zeros((96, samples), jnp.float32)], axis=0)
        vec[...] = jnp.transpose(full).astype(jnp.bfloat16)
        vsum[...] = jnp.dot(jnp.ones((8, samples), jnp.bfloat16), vec[...], preferred_element_type=jnp.float32)

    acc = jnp.dot(genotype[...], vec[...], preferred_element_type=jnp.float32)
    squares, bases = [], []
    for r in range(0, STEP, 64):
        base = jnp.broadcast_to(genotype[r : r + 64, 0:128].astype(jnp.float32)[:, 0:1], (64, 128))
        sq = jnp.zeros((64, 128), jnp.float32)
        for c in range(0, samples, 128):
            dev = genotype[r : r + 64, c : c + 128].astype(jnp.float32) - base
            sq = sq + dev * dev
        squares.append(jnp.sum(sq, axis=1, keepdims=True))
        bases.append(base)
    lane = lax.broadcasted_iota(jnp.int32, acc.shape, 1)
    acc = jnp.where(lane == SQUARES, jnp.concatenate(squares, axis=0), acc)
    acc = jnp.where(lane == VSUM, jnp.concatenate(bases, axis=0), acc)
    flat = jnp.transpose(acc)[0:ROWS, :]
    mean = flat[MEAN : MEAN + 1] / samples
    apart = mean - flat[VSUM : VSUM + 1]
    spread = jnp.maximum(flat[SQUARES : SQUARES + 1] - samples * apart * apart, 0.0)
    row = lax.broadcasted_iota(jnp.int32, flat.shape, 0)
    total = jnp.concatenate([vsum[0:1, :]] * (STEP // 128), axis=1)
    flat = jnp.where(row == MEAN, mean, jnp.where(row == SQUARES, spread, flat))
    out[0] = jnp.where(row == VSUM, total, flat)


def local_stats(probes, phenotype, genotype):
    variants, samples = genotype.shape
    half = variants // 2 // STEP
    return pl.pallas_call(
        stats_kernel,
        grid=(variants // STEP,),
        in_specs=[
            pl.BlockSpec((NV - 1, samples), lambda i: (0, 0)),
            pl.BlockSpec((1, samples), lambda i: (0, 0)),
            pl.BlockSpec((STEP, samples), lambda i: (i, 0)),
        ],
        out_specs=pl.BlockSpec((1, ROWS, STEP), lambda i: (i // half, 0, i % half)),
        out_shape=jax.ShapeDtypeStruct((2, ROWS, variants // 2), jnp.float32),
        scratch_shapes=[pltpu.VMEM((samples, 128), jnp.bfloat16), pltpu.VMEM((8, 128), jnp.float32)],
        compiler_params=pltpu.CompilerParams(vmem_limit_bytes=56 * 1024 * 1024),
        name="local_stats",
    )(probes, phenotype, genotype)


def merged(pieces, each):
    total = sum(pieces[1:], pieces[0])
    mean = total[MEAN : MEAN + 1] * (1.0 / len(pieces))
    apart = sum((p[MEAN : MEAN + 1] - mean) ** 2 for p in pieces) * each
    row = lax.broadcasted_iota(jnp.int32, total.shape, 0)
    return jnp.where(row == MEAN, mean, jnp.where(row == SQUARES, total + apart, total))


def over_samples(stats, samples):
    zlo = lax.axis_index("smp") // 4
    mine = lax.dynamic_index_in_dim(stats, zlo, 0, keepdims=False)
    other = lax.dynamic_index_in_dim(stats, 1 - zlo, 0, keepdims=False)
    own = merged([mine, shifted(other, "smp", ZLO_SWAP)], samples)
    below = shifted(own, "smp", X_UP)
    above = shifted(own, "smp", X_DOWN)
    cut = own.shape[1] // 2
    far_low = shifted(below[:, :cut], "smp", X_UP)
    far_high = shifted(above[:, cut:], "smp", X_DOWN)
    far = jnp.concatenate([far_low, far_high], axis=1)
    own = merged([own, below, above, far], 2 * samples)
    back = shifted(own, "smp", ZLO_SWAP)
    return jnp.where(zlo == 0, own, back), jnp.where(zlo == 0, back, own)


PAIRS = NV // 2
PACK = 88


def terms_kernel(place, low, high, labels, genotype, keep, give, weights, shift):
    variants, samples = genotype.shape
    stats = jnp.concatenate([low[...], high[...]], axis=1)
    mean = stats[MEAN : MEAN + 1]
    scale = lax.rsqrt(stats[SQUARES : SQUARES + 1] / N + EPS)
    sub = lax.broadcasted_iota(jnp.int32, (ROWS, 128), 0)
    lane = lax.broadcasted_iota(jnp.int32, (ROWS, 128), 1)
    vsum = jnp.sum(jnp.where(sub == lane, stats[VSUM : VSUM + 1, 0:128], 0.0), axis=1, keepdims=True)
    projected = (stats - vsum * mean) * scale
    weight = projected * scale
    comp = lax.broadcasted_iota(jnp.int32, (K, variants), 0)
    member = comp == labels[...]
    counts = jnp.sum(jnp.where(member, 1.0, 0.0), axis=1, keepdims=True)

    def rows_of(array, j):
        return jnp.where(member, array[j : j + 1], 0.0)

    for pair in range(PAIRS + 1):
        first = rows_of(weight, 2 * pair)
        second = rows_of(weight, 2 * pair + 1) if pair < PAIRS else jnp.zeros_like(first)
        weights[16 * pair : 16 * pair + 16, :] = jnp.concatenate([first, second], axis=0).astype(jnp.bfloat16)
    for r in range(0, 2 * PACK, 16):
        held = weights[r : r + 16, :].astype(jnp.float32)
        shift[r : r + 16, :] = jnp.broadcast_to(jnp.sum(held * mean, axis=1, keepdims=True), (16, 128))
    shift[K * NV :, :] = jnp.broadcast_to(-counts, (K, 128))

    spot = place[0]
    y, z, core = spot // 8, (spot // 2) % 4, spot % 2
    low_lanes = lax.broadcasted_iota(jnp.int32, (PACK, 128), 1) < 64
    for c in range(samples // 256):
        block = jnp.dot(weights[...], genotype[:, 256 * c : 256 * c + 256], preferred_element_type=jnp.float32)
        for h in range(2):
            t = 2 * c + h
            tile = block[:, 128 * h : 128 * h + 128] - shift[...]
            a, b = tile[:PACK], tile[PACK:]
            ra, rb = pltpu.roll(a, 64, 1), pltpu.roll(b, 64, 1)
            zero = jnp.where(low_lanes, a, rb)
            one = jnp.where(low_lanes, ra, b)
            ky, kz = (t // 4 - y + 4) % 4, (t % 4 - z + 4) % 4
            keep[ky, kz] = jnp.where(core == 0, zero, one)
            give[ky, kz] = jnp.where(core == 0, one, zero)


def local_terms(place, low, high, labels, genotype):
    vmem = pl.BlockSpec(memory_space=pltpu.VMEM)
    tiles = jax.ShapeDtypeStruct((4, 4, PACK, 128), jnp.float32)
    variants = genotype.shape[0]
    return pl.pallas_call(
        terms_kernel,
        in_specs=[pl.BlockSpec(memory_space=pltpu.SMEM), vmem, vmem, vmem, vmem],
        out_specs=(vmem, vmem),
        out_shape=(tiles, tiles),
        scratch_shapes=[pltpu.VMEM((2 * PACK, variants), jnp.bfloat16), pltpu.VMEM((2 * PACK, 128), jnp.float32)],
        compiler_params=pltpu.CompilerParams(vmem_limit_bytes=16 * 1024 * 1024),
        name="local_terms",
    )(place, low, high, labels, genotype)


def direct_sum(parts, axis, up, across, down):
    here, above, far, below = parts
    return here + shifted(above, axis, up) + shifted(below, axis, down) + shifted(far, axis, across)


def over_variants(keep, give):
    whole = keep + shifted(give, "var", CORE_SWAP)
    column = direct_sum([whole[k] for k in range(4)], "var", Y_UP, Y_ACROSS, Y_DOWN)
    return direct_sum([column[k] for k in range(4)], "var", Z_UP, Z_ACROSS, Z_DOWN)


def body(genotype, labels, probes, phenotype):
    variants, samples = genotype.shape
    stats = local_stats(probes, phenotype.astype(jnp.float32).reshape(1, samples), genotype)
    low, high = over_samples(stats, samples)
    place = lax.axis_index("var").astype(jnp.int32).reshape(1)
    keep, give = local_terms(place, low, high, labels.reshape(1, variants), genotype)
    packed = over_variants(keep, give)
    rows = jnp.concatenate([packed[:, :64], packed[:, 64:]], axis=0).reshape(NV + 1, K, 64)
    out = rows[:NV] / rows[NV:]
    return jnp.transpose(out, (1, 0, 2)).reshape(K, NV, 1, 64)


def solution(mesh):
    placed = (P("var", "smp"), P("var"), P(None, "smp"), P("smp"))
    return jax.shard_map(
        body, mesh=mesh, in_specs=placed, out_specs=P(None, None, "smp", "var"), check_vma=False
    )
```

```python
import jax
import jax.numpy as jnp
from jax import lax
from jax.experimental import pallas as pl
from jax.experimental.pallas import tpu as pltpu
from jax.sharding import PartitionSpec as P

K = 8
NV = 21
EPS = 1e-06
N = 16384

MEAN, SQUARES, VSUM = 21, 22, 23
ROWS = 24
STEP = 256


def shifted(array, axis, perm):
    return lax.ppermute(array, axis, perm)


ZLO_SWAP = [(i, i ^ 4) for i in range(8)]
X_UP = [(i, (i & 4) | ((i + 1) & 3)) for i in range(8)]
X_DOWN = [(i, (i & 4) | ((i - 1) & 3)) for i in range(8)]
CORE_SWAP = [(i, i ^ 1) for i in range(32)]
Y_UP = [(i, (i + 8) % 32) for i in range(32)]
Y_ACROSS = [(i, (i + 16) % 32) for i in range(32)]
Y_DOWN = [(i, (i - 8) % 32) for i in range(32)]
Z_UP = [(i, (i & 25) | ((i + 2) & 6)) for i in range(32)]
Z_ACROSS = [(i, i ^ 4) for i in range(32)]
Z_DOWN = [(i, (i & 25) | ((i - 2) & 6)) for i in range(32)]


def stats_kernel(place, probes, phenotype, genotype, held, mine, other, vec, vsum, arrived):
    variants, samples = genotype.shape
    steps = variants // STEP
    zlo = (place[0] // 4) % 2

    def copy(i):
        rows = pl.ds(pl.multiple_of(i * STEP, STEP), STEP)
        return pltpu.make_async_copy(genotype.at[rows], held.at[rows], arrived.at[i])

    for i in range(steps):
        copy(i).start()
    row = lax.broadcasted_iota(jnp.int32, (32, samples), 0)
    low = jnp.concatenate([probes[...].astype(jnp.float32), jnp.zeros((12, samples), jnp.float32)], axis=0)
    phen = phenotype[...].astype(jnp.float32).reshape(1, samples)
    low = jnp.where(row == NV - 1, phen, jnp.where(row == MEAN, 1.0, low))
    full = jnp.concatenate([low, jnp.zeros((96, samples), jnp.float32)], axis=0)
    vec[...] = jnp.transpose(full).astype(jnp.bfloat16)
    vsum[...] = jnp.dot(jnp.ones((8, samples), jnp.bfloat16), vec[...], preferred_element_type=jnp.float32)

    def step(i, carry):
        copy(i).wait()
        rows = pl.ds(pl.multiple_of(i * STEP, STEP), STEP)
        acc = jnp.dot(held[rows, :], vec[...], preferred_element_type=jnp.float32)
        squares, bases = [], []
        for r in range(0, STEP, 64):
            part = pl.ds(pl.multiple_of(i * STEP + r, 64), 64)
            base = jnp.broadcast_to(held[part, 0:128].astype(jnp.float32)[:, 0:1], (64, 128))
            sq = jnp.zeros((64, 128), jnp.float32)
            for c in range(0, samples, 128):
                dev = held[part, c : c + 128].astype(jnp.float32) - base
                sq = sq + dev * dev
            squares.append(jnp.sum(sq, axis=1, keepdims=True))
            bases.append(base)
        lane = lax.broadcasted_iota(jnp.int32, acc.shape, 1)
        acc = jnp.where(lane == SQUARES, jnp.concatenate(squares, axis=0), acc)
        acc = jnp.where(lane == VSUM, jnp.concatenate(bases, axis=0), acc)
        flat = jnp.transpose(acc)[0:ROWS, :]
        mean = flat[MEAN : MEAN + 1] / samples
        apart = mean - flat[VSUM : VSUM + 1]
        spread = jnp.maximum(flat[SQUARES : SQUARES + 1] - samples * apart * apart, 0.0)
        row = lax.broadcasted_iota(jnp.int32, flat.shape, 0)
        total = jnp.concatenate([vsum[0:1, :]] * (STEP // 128), axis=1)
        flat = jnp.where(row == MEAN, mean, jnp.where(row == SQUARES, spread, flat))
        flat = jnp.where(row == VSUM, total, flat)
        half = steps // 2
        spot = pl.ds(pl.multiple_of((i % half) * STEP, STEP), STEP)
        own = (i // half) == zlo

        @pl.when(own)
        def _():
            mine[:, spot] = flat

        @pl.when(jnp.logical_not(own))
        def _():
            other[:, spot] = flat

        return carry

    lax.fori_loop(0, steps, step, 0)


def local_stats(place, probes, phenotype, genotype):
    variants, samples = genotype.shape
    vmem = pl.BlockSpec(memory_space=pltpu.VMEM)
    block = jax.ShapeDtypeStruct((ROWS, variants // 2), jnp.float32)
    return pl.pallas_call(
        stats_kernel,
        in_specs=[pl.BlockSpec(memory_space=pltpu.SMEM), vmem, vmem, pl.BlockSpec(memory_space=pltpu.HBM)],
        out_specs=(vmem, vmem, vmem),
        out_shape=(jax.ShapeDtypeStruct(genotype.shape, genotype.dtype), block, block),
        scratch_shapes=[
            pltpu.VMEM((samples, 128), jnp.bfloat16),
            pltpu.VMEM((8, 128), jnp.float32),
            pltpu.SemaphoreType.DMA((variants // STEP,)),
        ],
        compiler_params=pltpu.CompilerParams(vmem_limit_bytes=40 * 1024 * 1024),
        name="local_stats",
    )(place, probes, phenotype, genotype)


def merged(pieces, each):
    total = sum(pieces[1:], pieces[0])
    mean = total[MEAN : MEAN + 1] * (1.0 / len(pieces))
    apart = sum((p[MEAN : MEAN + 1] - mean) ** 2 for p in pieces) * each
    row = lax.broadcasted_iota(jnp.int32, total.shape, 0)
    return jnp.where(row == MEAN, mean, jnp.where(row == SQUARES, total + apart, total))


def over_samples(mine, other, samples):
    own = merged([mine, shifted(other, "smp", ZLO_SWAP)], samples)
    below = shifted(own, "smp", X_UP)
    above = shifted(own, "smp", X_DOWN)
    cut = own.shape[1] // 2
    far_low = shifted(below[:, :cut], "smp", X_UP)
    far_high = shifted(above[:, cut:], "smp", X_DOWN)
    far = jnp.concatenate([far_low, far_high], axis=1)
    own = merged([own, below, above, far], 2 * samples)
    return own, shifted(own, "smp", ZLO_SWAP)


PAIRS = NV // 2
PACK = 88


def terms_kernel(place, own, back, labels, genotype, keep, give, weights, shift):
    variants, samples = genotype.shape
    lower = (place[0] // 4) % 2 == 0
    stats = jnp.concatenate(
        [jnp.where(lower, own[...], back[...]), jnp.where(lower, back[...], own[...])], axis=1
    )
    mean = stats[MEAN : MEAN + 1]
    scale = lax.rsqrt(stats[SQUARES : SQUARES + 1] / N + EPS)
    sub = lax.broadcasted_iota(jnp.int32, (ROWS, 128), 0)
    lane = lax.broadcasted_iota(jnp.int32, (ROWS, 128), 1)
    vsum = jnp.sum(jnp.where(sub == lane, stats[VSUM : VSUM + 1, 0:128], 0.0), axis=1, keepdims=True)
    projected = (stats - vsum * mean) * scale
    weight = projected * scale
    comp = lax.broadcasted_iota(jnp.int32, (K, variants), 0)
    member = comp == labels[...]
    counts = jnp.sum(jnp.where(member, 1.0, 0.0), axis=1, keepdims=True)

    def rows_of(array, j):
        return jnp.where(member, array[j : j + 1], 0.0)

    for pair in range(PAIRS + 1):
        first = rows_of(weight, 2 * pair)
        second = rows_of(weight, 2 * pair + 1) if pair < PAIRS else jnp.zeros_like(first)
        weights[16 * pair : 16 * pair + 16, :] = jnp.concatenate([first, second], axis=0).astype(jnp.bfloat16)
    for r in range(0, 2 * PACK, 16):
        held = weights[r : r + 16, :].astype(jnp.float32)
        shift[r : r + 16, :] = jnp.broadcast_to(jnp.sum(held * mean, axis=1, keepdims=True), (16, 128))
    shift[K * NV :, :] = jnp.broadcast_to(-counts, (K, 128))

    spot = place[0] // 8
    y, z, core = spot // 8, (spot // 2) % 4, spot % 2
    low_lanes = lax.broadcasted_iota(jnp.int32, (PACK, 128), 1) < 64
    for c in range(samples // 256):
        block = jnp.dot(weights[...], genotype[:, 256 * c : 256 * c + 256], preferred_element_type=jnp.float32)
        for h in range(2):
            t = 2 * c + h
            tile = block[:, 128 * h : 128 * h + 128] - shift[...]
            a, b = tile[:PACK], tile[PACK:]
            ra, rb = pltpu.roll(a, 64, 1), pltpu.roll(b, 64, 1)
            zero = jnp.where(low_lanes, a, rb)
            one = jnp.where(low_lanes, ra, b)
            ky, kz = (t // 4 - y + 4) % 4, (t % 4 - z + 4) % 4
            keep[ky, kz] = jnp.where(core == 0, zero, one)
            give[ky, kz] = jnp.where(core == 0, one, zero)


def local_terms(place, own, back, labels, genotype):
    vmem = pl.BlockSpec(memory_space=pltpu.VMEM)
    tiles = jax.ShapeDtypeStruct((4, 4, PACK, 128), jnp.float32)
    variants = genotype.shape[0]
    return pl.pallas_call(
        terms_kernel,
        in_specs=[pl.BlockSpec(memory_space=pltpu.SMEM), vmem, vmem, vmem, vmem],
        out_specs=(vmem, vmem),
        out_shape=(tiles, tiles),
        scratch_shapes=[pltpu.VMEM((2 * PACK, variants), jnp.bfloat16), pltpu.VMEM((2 * PACK, 128), jnp.float32)],
        compiler_params=pltpu.CompilerParams(vmem_limit_bytes=16 * 1024 * 1024),
        name="local_terms",
    )(place, own, back, labels, genotype)


def direct_sum(parts, axis, up, across, down):
    here, above, far, below = parts
    return here + shifted(above, axis, up) + shifted(below, axis, down) + shifted(far, axis, across)


def over_variants(keep, give):
    whole = keep + shifted(give, "var", CORE_SWAP)
    column = direct_sum([whole[k] for k in range(4)], "var", Y_UP, Y_ACROSS, Y_DOWN)
    return direct_sum([column[k] for k in range(4)], "var", Z_UP, Z_ACROSS, Z_DOWN)


def body(genotype, labels, probes, phenotype):
    variants, samples = genotype.shape
    place = lax.axis_index(("var", "smp")).astype(jnp.int32).reshape(1)
    held, mine, other = local_stats(place, probes, phenotype, genotype)
    own, back = over_samples(mine, other, samples)
    keep, give = local_terms(place, own, back, labels.reshape(1, variants), held)
    packed = over_variants(keep, give)
    rows = jnp.concatenate([packed[:, :64], packed[:, 64:]], axis=0).reshape(NV + 1, K, 64)
    out = rows[:NV] / rows[NV:]
    return jnp.transpose(out, (1, 0, 2)).reshape(K, NV, 1, 64)


def solution(mesh):
    placed = (P("var", "smp"), P("var"), P(None, "smp"), P("smp"))
    return jax.shard_map(
        body, mesh=mesh, in_specs=placed, out_specs=P(None, None, "smp", "var"), check_vma=False
    )
```

```python
import jax
import jax.numpy as jnp
from jax import lax
from jax.experimental import pallas as pl
from jax.experimental.pallas import tpu as pltpu
from jax.sharding import PartitionSpec as P

K = 8
NV = 21
EPS = 1e-06
N = 16384

MEAN, SQUARES, VSUM = 21, 22, 23
ROWS = 24
STEP = 256


def shifted(array, axis, perm):
    return lax.ppermute(array, axis, perm)


ZLO_SWAP = [(i, i ^ 4) for i in range(8)]
X_SWAP = [(i, i ^ 1) for i in range(8)]
X_TURN = [(i, i ^ 3) for i in range(8)]
CORE_SWAP = [(i, i ^ 1) for i in range(32)]
Y_UP = [(i, (i + 8) % 32) for i in range(32)]
Y_ACROSS = [(i, (i + 16) % 32) for i in range(32)]
Y_DOWN = [(i, (i - 8) % 32) for i in range(32)]
Z_UP = [(i, (i & 25) | ((i + 2) & 6)) for i in range(32)]
Z_ACROSS = [(i, i ^ 4) for i in range(32)]
Z_DOWN = [(i, (i & 25) | ((i - 2) & 6)) for i in range(32)]


def stats_kernel(place, probes, phenotype, genotype, held, mine, other, vec, vsum, arrived):
    variants, samples = genotype.shape
    steps = variants // STEP
    zlo = (place[0] // 4) % 2

    def copy(i):
        rows = pl.ds(pl.multiple_of(i * STEP, STEP), STEP)
        return pltpu.make_async_copy(genotype.at[rows], held.at[rows], arrived.at[i])

    for i in range(steps):
        copy(i).start()
    row = lax.broadcasted_iota(jnp.int32, (32, samples), 0)
    low = jnp.concatenate([probes[...].astype(jnp.float32), jnp.zeros((12, samples), jnp.float32)], axis=0)
    phen = phenotype[...].astype(jnp.float32).reshape(1, samples)
    low = jnp.where(row == NV - 1, phen, jnp.where(row == MEAN, 1.0, low))
    full = jnp.concatenate([low, jnp.zeros((96, samples), jnp.float32)], axis=0)
    vec[...] = jnp.transpose(full).astype(jnp.bfloat16)
    vsum[...] = jnp.dot(jnp.ones((8, samples), jnp.bfloat16), vec[...], preferred_element_type=jnp.float32)

    def step(i, carry):
        copy(i).wait()
        rows = pl.ds(pl.multiple_of(i * STEP, STEP), STEP)
        acc = jnp.dot(held[rows, :], vec[...], preferred_element_type=jnp.float32)
        squares, bases = [], []
        for r in range(0, STEP, 64):
            part = pl.ds(pl.multiple_of(i * STEP + r, 64), 64)
            base = jnp.broadcast_to(held[part, 0:128].astype(jnp.float32)[:, 0:1], (64, 128))
            sq = jnp.zeros((64, 128), jnp.float32)
            for c in range(0, samples, 128):
                dev = held[part, c : c + 128].astype(jnp.float32) - base
                sq = sq + dev * dev
            squares.append(jnp.sum(sq, axis=1, keepdims=True))
            bases.append(base)
        lane = lax.broadcasted_iota(jnp.int32, acc.shape, 1)
        acc = jnp.where(lane == SQUARES, jnp.concatenate(squares, axis=0), acc)
        acc = jnp.where(lane == VSUM, jnp.concatenate(bases, axis=0), acc)
        flat = jnp.transpose(acc)[0:ROWS, :]
        mean = flat[MEAN : MEAN + 1] / samples
        apart = mean - flat[VSUM : VSUM + 1]
        spread = jnp.maximum(flat[SQUARES : SQUARES + 1] - samples * apart * apart, 0.0)
        row = lax.broadcasted_iota(jnp.int32, flat.shape, 0)
        total = jnp.concatenate([vsum[0:1, :]] * (STEP // 128), axis=1)
        flat = jnp.where(row == MEAN, mean, jnp.where(row == SQUARES, spread, flat))
        flat = jnp.where(row == VSUM, total, flat)
        half = steps // 2
        spot = pl.ds(pl.multiple_of((i % half) * STEP, STEP), STEP)
        own = (i // half) == zlo

        @pl.when(own)
        def _():
            mine[:, spot] = flat

        @pl.when(jnp.logical_not(own))
        def _():
            other[:, spot] = flat

        return carry

    lax.fori_loop(0, steps, step, 0)


def local_stats(place, probes, phenotype, genotype):
    variants, samples = genotype.shape
    vmem = pl.BlockSpec(memory_space=pltpu.VMEM)
    block = jax.ShapeDtypeStruct((ROWS, variants // 2), jnp.float32)
    return pl.pallas_call(
        stats_kernel,
        in_specs=[pl.BlockSpec(memory_space=pltpu.SMEM), vmem, vmem, pl.BlockSpec(memory_space=pltpu.HBM)],
        out_specs=(vmem, vmem, vmem),
        out_shape=(jax.ShapeDtypeStruct(genotype.shape, genotype.dtype), block, block),
        scratch_shapes=[
            pltpu.VMEM((samples, 128), jnp.bfloat16),
            pltpu.VMEM((8, 128), jnp.float32),
            pltpu.SemaphoreType.DMA((variants // STEP,)),
        ],
        compiler_params=pltpu.CompilerParams(vmem_limit_bytes=40 * 1024 * 1024),
        name="local_stats",
    )(place, probes, phenotype, genotype)


def merged(pieces, each):
    total = sum(pieces[1:], pieces[0])
    mean = total[MEAN : MEAN + 1] * (1.0 / len(pieces))
    apart = sum((p[MEAN : MEAN + 1] - mean) ** 2 for p in pieces) * each
    row = lax.broadcasted_iota(jnp.int32, total.shape, 0)
    return jnp.where(row == MEAN, mean, jnp.where(row == SQUARES, total + apart, total))


def over_samples(mine, other, samples):
    own = merged([mine, shifted(other, "smp", ZLO_SWAP)], samples)
    own = merged([own, shifted(own, "smp", X_SWAP)], 2 * samples)
    own = merged([own, shifted(own, "smp", X_TURN)], 4 * samples)
    return own, shifted(own, "smp", ZLO_SWAP)


PAIRS = NV // 2
PACK = 88
CUT = 48


def terms_kernel(place, own, back, labels, genotype, keep_a, keep_b, give_a, give_b, weights, shift):
    variants, samples = genotype.shape
    lower = (place[0] // 4) % 2 == 0
    stats = jnp.concatenate(
        [jnp.where(lower, own[...], back[...]), jnp.where(lower, back[...], own[...])], axis=1
    )
    mean = stats[MEAN : MEAN + 1]
    scale = lax.rsqrt(stats[SQUARES : SQUARES + 1] / N + EPS)
    sub = lax.broadcasted_iota(jnp.int32, (ROWS, 128), 0)
    lane = lax.broadcasted_iota(jnp.int32, (ROWS, 128), 1)
    vsum = jnp.sum(jnp.where(sub == lane, stats[VSUM : VSUM + 1, 0:128], 0.0), axis=1, keepdims=True)
    projected = (stats - vsum * mean) * scale
    weight = projected * scale
    comp = lax.broadcasted_iota(jnp.int32, (K, variants), 0)
    member = comp == labels[...]
    counts = jnp.sum(jnp.where(member, 1.0, 0.0), axis=1, keepdims=True)

    def rows_of(array, j):
        return jnp.where(member, array[j : j + 1], 0.0)

    for pair in range(PAIRS + 1):
        first = rows_of(weight, 2 * pair)
        second = rows_of(weight, 2 * pair + 1) if pair < PAIRS else jnp.zeros_like(first)
        weights[16 * pair : 16 * pair + 16, :] = jnp.concatenate([first, second], axis=0).astype(jnp.bfloat16)
    for r in range(0, 2 * PACK, 16):
        held = weights[r : r + 16, :].astype(jnp.float32)
        shift[r : r + 16, :] = jnp.broadcast_to(jnp.sum(held * mean, axis=1, keepdims=True), (16, 128))
    shift[K * NV :, :] = jnp.broadcast_to(-counts, (K, 128))

    spot = place[0] // 8
    y, z, core = spot // 8, (spot // 2) % 4, spot % 2
    low_lanes = lax.broadcasted_iota(jnp.int32, (PACK, 128), 1) < 64
    for c in range(samples // 256):
        block = jnp.dot(weights[...], genotype[:, 256 * c : 256 * c + 256], preferred_element_type=jnp.float32)
        for h in range(2):
            t = 2 * c + h
            tile = block[:, 128 * h : 128 * h + 128] - shift[...]
            a, b = tile[:PACK], tile[PACK:]
            ra, rb = pltpu.roll(a, 64, 1), pltpu.roll(b, 64, 1)
            zero = jnp.where(low_lanes, a, rb)
            one = jnp.where(low_lanes, ra, b)
            ky, kz = (t // 4 - y + 4) % 4, (t % 4 - z + 4) % 4
            keep = jnp.where(core == 0, zero, one)
            give = jnp.where(core == 0, one, zero)
            keep_a[ky, kz], keep_b[ky, kz] = keep[:CUT], keep[CUT:]
            give_a[ky, kz], give_b[ky, kz] = give[:CUT], give[CUT:]


def local_terms(place, own, back, labels, genotype):
    vmem = pl.BlockSpec(memory_space=pltpu.VMEM)
    upper = jax.ShapeDtypeStruct((4, 4, CUT, 128), jnp.float32)
    lower = jax.ShapeDtypeStruct((4, 4, PACK - CUT, 128), jnp.float32)
    variants = genotype.shape[0]
    return pl.pallas_call(
        terms_kernel,
        in_specs=[pl.BlockSpec(memory_space=pltpu.SMEM), vmem, vmem, vmem, vmem],
        out_specs=(vmem, vmem, vmem, vmem),
        out_shape=(upper, lower, upper, lower),
        scratch_shapes=[pltpu.VMEM((2 * PACK, variants), jnp.bfloat16), pltpu.VMEM((2 * PACK, 128), jnp.float32)],
        compiler_params=pltpu.CompilerParams(vmem_limit_bytes=16 * 1024 * 1024),
        name="local_terms",
    )(place, own, back, labels, genotype)


def direct_sum(parts, axis, up, across, down):
    here, above, far, below = parts
    return here + shifted(above, axis, up) + shifted(below, axis, down) + shifted(far, axis, across)


def over_variants(keep, give):
    whole = keep + shifted(give, "var", CORE_SWAP)
    column = direct_sum([whole[k] for k in range(4)], "var", Y_UP, Y_ACROSS, Y_DOWN)
    return direct_sum([column[k] for k in range(4)], "var", Z_UP, Z_ACROSS, Z_DOWN)


def body(genotype, labels, probes, phenotype):
    variants, samples = genotype.shape
    place = lax.axis_index(("var", "smp")).astype(jnp.int32).reshape(1)
    held, mine, other = local_stats(place, probes, phenotype, genotype)
    own, back = over_samples(mine, other, samples)
    keep_a, keep_b, give_a, give_b = local_terms(place, own, back, labels.reshape(1, variants), held)
    packed = jnp.concatenate([over_variants(keep_a, give_a), over_variants(keep_b, give_b)], axis=0)
    rows = jnp.concatenate([packed[:, :64], packed[:, 64:]], axis=0).reshape(NV + 1, K, 64)
    out = rows[:NV] / rows[NV:]
    return jnp.transpose(out, (1, 0, 2)).reshape(K, NV, 1, 64)


def solution(mesh):
    placed = (P("var", "smp"), P("var"), P(None, "smp"), P("smp"))
    return jax.shard_map(
        body, mesh=mesh, in_specs=placed, out_specs=P(None, None, "smp", "var"), check_vma=False
    )
```

```python
import jax
import jax.numpy as jnp
from jax import lax
from jax.experimental import pallas as pl
from jax.experimental.pallas import tpu as pltpu
from jax.sharding import PartitionSpec as P

K = 8
NV = 21
EPS = 1e-06
N = 16384

MEAN, SQUARES, VSUM = 21, 22, 23
ROWS = 24
STEP = 256


def shifted(array, axis, perm):
    return lax.ppermute(array, axis, perm)


ZLO_SWAP = [(i, i ^ 4) for i in range(8)]
X_SWAP = [(i, i ^ 1) for i in range(8)]
X_TURN = [(i, i ^ 3) for i in range(8)]
CORE_SWAP = [(i, i ^ 1) for i in range(32)]
Y_UP = [(i, (i + 8) % 32) for i in range(32)]
Y_ACROSS = [(i, (i + 16) % 32) for i in range(32)]
Y_DOWN = [(i, (i - 8) % 32) for i in range(32)]
Z_UP = [(i, (i & 25) | ((i + 2) & 6)) for i in range(32)]
Z_ACROSS = [(i, i ^ 4) for i in range(32)]
Z_DOWN = [(i, (i & 25) | ((i - 2) & 6)) for i in range(32)]


def block_stats(held, first, vec, vsum):
    samples = held.shape[1]
    rows = pl.ds(pl.multiple_of(first, STEP), STEP)
    acc = jnp.dot(held[rows, :], vec[...], preferred_element_type=jnp.float32)
    squares, bases = [], []
    for r in range(0, STEP, 64):
        part = pl.ds(pl.multiple_of(first + r, 64), 64)
        base = jnp.broadcast_to(held[part, 0:128].astype(jnp.float32)[:, 0:1], (64, 128))
        sq = jnp.zeros((64, 128), jnp.float32)
        for c in range(0, samples, 128):
            dev = held[part, c : c + 128].astype(jnp.float32) - base
            sq = sq + dev * dev
        squares.append(jnp.sum(sq, axis=1, keepdims=True))
        bases.append(base)
    lane = lax.broadcasted_iota(jnp.int32, acc.shape, 1)
    acc = jnp.where(lane == SQUARES, jnp.concatenate(squares, axis=0), acc)
    acc = jnp.where(lane == VSUM, jnp.concatenate(bases, axis=0), acc)
    flat = jnp.transpose(acc)[0:ROWS, :]
    mean = flat[MEAN : MEAN + 1] / samples
    apart = mean - flat[VSUM : VSUM + 1]
    spread = jnp.maximum(flat[SQUARES : SQUARES + 1] - samples * apart * apart, 0.0)
    row = lax.broadcasted_iota(jnp.int32, flat.shape, 0)
    total = jnp.concatenate([vsum[0:1, :]] * (STEP // 128), axis=1)
    flat = jnp.where(row == MEAN, mean, jnp.where(row == SQUARES, spread, flat))
    return jnp.where(row == VSUM, total, flat)


def first_kernel(place, probes, phenotype, genotype, held, other, vec, vsum, arrived):
    variants, samples = genotype.shape
    steps = variants // STEP
    ahead = steps // 2
    away = (1 - (place[0] // 4) % 2) * ahead

    def copy(i):
        source = pl.ds(pl.multiple_of(((i + away) % steps) * STEP, STEP), STEP)
        target = pl.ds(pl.multiple_of(i * STEP, STEP), STEP)
        return pltpu.make_async_copy(genotype.at[source], held.at[target], arrived.at[i])

    for i in range(ahead):
        copy(i).start()
    row = lax.broadcasted_iota(jnp.int32, (32, samples), 0)
    low = jnp.concatenate([probes[...].astype(jnp.float32), jnp.zeros((12, samples), jnp.float32)], axis=0)
    phen = phenotype[...].astype(jnp.float32).reshape(1, samples)
    low = jnp.where(row == NV - 1, phen, jnp.where(row == MEAN, 1.0, low))
    full = jnp.concatenate([low, jnp.zeros((96, samples), jnp.float32)], axis=0)
    vec[...] = jnp.transpose(full).astype(jnp.bfloat16)
    vsum[...] = jnp.dot(jnp.ones((8, samples), jnp.bfloat16), vec[...], preferred_element_type=jnp.float32)

    def step(i, carry):
        copy(i).wait()
        copy(i + ahead).start()
        other[:, pl.ds(pl.multiple_of(i * STEP, STEP), STEP)] = block_stats(held, i * STEP, vec, vsum)
        return carry

    lax.fori_loop(0, ahead, step, 0)
    for i in range(ahead, steps):
        copy(i).wait()


def second_kernel(held, vec, vsum, mine):
    half = held.shape[0] // 2

    def step(i, carry):
        mine[:, pl.ds(pl.multiple_of(i * STEP, STEP), STEP)] = block_stats(held, half + i * STEP, vec, vsum)
        return carry

    lax.fori_loop(0, half // STEP, step, 0)


def local_stats(place, probes, phenotype, genotype):
    variants, samples = genotype.shape
    vmem = pl.BlockSpec(memory_space=pltpu.VMEM)
    block = jax.ShapeDtypeStruct((ROWS, variants // 2), jnp.float32)
    held, other, vec, vsum = pl.pallas_call(
        first_kernel,
        in_specs=[pl.BlockSpec(memory_space=pltpu.SMEM), vmem, vmem, pl.BlockSpec(memory_space=pltpu.HBM)],
        out_specs=(vmem, vmem, vmem, vmem),
        out_shape=(
            jax.ShapeDtypeStruct(genotype.shape, genotype.dtype),
            block,
            jax.ShapeDtypeStruct((samples, 128), jnp.bfloat16),
            jax.ShapeDtypeStruct((8, 128), jnp.float32),
        ),
        scratch_shapes=[pltpu.SemaphoreType.DMA((variants // STEP,))],
        compiler_params=pltpu.CompilerParams(vmem_limit_bytes=40 * 1024 * 1024),
        name="first_stats",
    )(place, probes, phenotype, genotype)
    theirs = shifted(other, "smp", ZLO_SWAP)
    mine = pl.pallas_call(
        second_kernel,
        in_specs=[vmem, vmem, vmem],
        out_specs=vmem,
        out_shape=block,
        compiler_params=pltpu.CompilerParams(vmem_limit_bytes=16 * 1024 * 1024),
        name="second_stats",
    )(held, vec, vsum)
    return held, mine, theirs


def merged(pieces, each):
    total = sum(pieces[1:], pieces[0])
    mean = total[MEAN : MEAN + 1] * (1.0 / len(pieces))
    apart = sum((p[MEAN : MEAN + 1] - mean) ** 2 for p in pieces) * each
    row = lax.broadcasted_iota(jnp.int32, total.shape, 0)
    return jnp.where(row == MEAN, mean, jnp.where(row == SQUARES, total + apart, total))


def over_samples(mine, theirs, samples):
    own = merged([mine, theirs], samples)
    own = merged([own, shifted(own, "smp", X_SWAP)], 2 * samples)
    own = merged([own, shifted(own, "smp", X_TURN)], 4 * samples)
    return own, shifted(own, "smp", ZLO_SWAP)


PAIRS = NV // 2
PACK = 88


def terms_kernel(place, own, back, labels, genotype, keep, give, weights, shift):
    variants, samples = genotype.shape
    half = variants // 2
    stats = jnp.concatenate([back[...], own[...]], axis=1)
    lower = (place[0] // 4) % 2 == 0
    tags = jnp.where(lower, jnp.concatenate([labels[:, half:], labels[:, :half]], axis=1), labels[...])
    mean = stats[MEAN : MEAN + 1]
    scale = lax.rsqrt(stats[SQUARES : SQUARES + 1] / N + EPS)
    sub = lax.broadcasted_iota(jnp.int32, (ROWS, 128), 0)
    lane = lax.broadcasted_iota(jnp.int32, (ROWS, 128), 1)
    vsum = jnp.sum(jnp.where(sub == lane, stats[VSUM : VSUM + 1, 0:128], 0.0), axis=1, keepdims=True)
    projected = (stats - vsum * mean) * scale
    weight = projected * scale
    comp = lax.broadcasted_iota(jnp.int32, (K, variants), 0)
    member = comp == tags
    counts = jnp.sum(jnp.where(member, 1.0, 0.0), axis=1, keepdims=True)

    def rows_of(array, j):
        return jnp.where(member, array[j : j + 1], 0.0)

    for pair in range(PAIRS + 1):
        first = rows_of(weight, 2 * pair)
        second = rows_of(weight, 2 * pair + 1) if pair < PAIRS else jnp.zeros_like(first)
        weights[16 * pair : 16 * pair + 16, :] = jnp.concatenate([first, second], axis=0).astype(jnp.bfloat16)
    for r in range(0, 2 * PACK, 16):
        held = weights[r : r + 16, :].astype(jnp.float32)
        shift[r : r + 16, :] = jnp.broadcast_to(jnp.sum(held * mean, axis=1, keepdims=True), (16, 128))
    shift[K * NV :, :] = jnp.broadcast_to(-counts, (K, 128))

    spot = place[0] // 8
    y, z, core = spot // 8, (spot // 2) % 4, spot % 2
    low_lanes = lax.broadcasted_iota(jnp.int32, (PACK, 128), 1) < 64
    for c in range(samples // 256):
        block = jnp.dot(weights[...], genotype[:, 256 * c : 256 * c + 256], preferred_element_type=jnp.float32)
        for h in range(2):
            t = 2 * c + h
            tile = block[:, 128 * h : 128 * h + 128] - shift[...]
            a, b = tile[:PACK], tile[PACK:]
            ra, rb = pltpu.roll(a, 64, 1), pltpu.roll(b, 64, 1)
            zero = jnp.where(low_lanes, a, rb)
            one = jnp.where(low_lanes, ra, b)
            ky, kz = (t // 4 - y + 4) % 4, (t % 4 - z + 4) % 4
            keep[ky, kz] = jnp.where(core == 0, zero, one)
            give[ky, kz] = jnp.where(core == 0, one, zero)


def local_terms(place, own, back, labels, genotype):
    vmem = pl.BlockSpec(memory_space=pltpu.VMEM)
    tiles = jax.ShapeDtypeStruct((4, 4, PACK, 128), jnp.float32)
    variants = genotype.shape[0]
    return pl.pallas_call(
        terms_kernel,
        in_specs=[pl.BlockSpec(memory_space=pltpu.SMEM), vmem, vmem, vmem, vmem],
        out_specs=(vmem, vmem),
        out_shape=(tiles, tiles),
        scratch_shapes=[pltpu.VMEM((2 * PACK, variants), jnp.bfloat16), pltpu.VMEM((2 * PACK, 128), jnp.float32)],
        compiler_params=pltpu.CompilerParams(vmem_limit_bytes=16 * 1024 * 1024),
        name="local_terms",
    )(place, own, back, labels, genotype)


def direct_sum(parts, axis, up, across, down):
    here, above, far, below = parts
    return here + shifted(above, axis, up) + shifted(below, axis, down) + shifted(far, axis, across)


def over_variants(keep, give):
    whole = keep + shifted(give, "var", CORE_SWAP)
    column = direct_sum([whole[k] for k in range(4)], "var", Y_UP, Y_ACROSS, Y_DOWN)
    return direct_sum([column[k] for k in range(4)], "var", Z_UP, Z_ACROSS, Z_DOWN)


def body(genotype, labels, probes, phenotype):
    variants, samples = genotype.shape
    place = lax.axis_index(("var", "smp")).astype(jnp.int32).reshape(1)
    held, mine, theirs = local_stats(place, probes, phenotype, genotype)
    own, back = over_samples(mine, theirs, samples)
    keep, give = local_terms(place, own, back, labels.reshape(1, variants), held)
    packed = over_variants(keep, give)
    rows = jnp.concatenate([packed[:, :64], packed[:, 64:]], axis=0).reshape(NV + 1, K, 64)
    out = rows[:NV] / rows[NV:]
    return jnp.transpose(out, (1, 0, 2)).reshape(K, NV, 1, 64)


def solution(mesh):
    placed = (P("var", "smp"), P("var"), P(None, "smp"), P("smp"))
    return jax.shard_map(
        body, mesh=mesh, in_specs=placed, out_specs=P(None, None, "smp", "var"), check_vma=False
    )
```

```python
import jax
import jax.numpy as jnp
from jax import lax
from jax.experimental import pallas as pl
from jax.experimental.pallas import tpu as pltpu
from jax.sharding import PartitionSpec as P

K = 8
NV = 21
EPS = 1e-06
N = 16384

MEAN, SQUARES, VSUM = 21, 22, 23
ROWS = 24
STEP = 256


def shifted(array, axis, perm):
    return lax.ppermute(array, axis, perm)


ZLO_SWAP = [(i, i ^ 4) for i in range(8)]
X_SWAP = [(i, i ^ 1) for i in range(8)]
X_TURN = [(i, i ^ 3) for i in range(8)]
CORE_SWAP = [(i, i ^ 1) for i in range(32)]
Y_UP = [(i, (i + 8) % 32) for i in range(32)]
Y_ACROSS = [(i, (i + 16) % 32) for i in range(32)]
Y_DOWN = [(i, (i - 8) % 32) for i in range(32)]
Z_UP = [(i, (i & 25) | ((i + 2) & 6)) for i in range(32)]
Z_ACROSS = [(i, i ^ 4) for i in range(32)]
Z_DOWN = [(i, (i & 25) | ((i - 2) & 6)) for i in range(32)]


def block_stats(held, first, vec, vsum):
    samples = held.shape[1]
    rows = pl.ds(pl.multiple_of(first, STEP), STEP)
    acc = jnp.dot(held[rows, :], vec[...], preferred_element_type=jnp.float32)
    squares, bases = [], []
    for r in range(0, STEP, 64):
        part = pl.ds(pl.multiple_of(first + r, 64), 64)
        base = jnp.broadcast_to(held[part, 0:128].astype(jnp.float32)[:, 0:1], (64, 128))
        sq = jnp.zeros((64, 128), jnp.float32)
        for c in range(0, samples, 128):
            dev = held[part, c : c + 128].astype(jnp.float32) - base
            sq = sq + dev * dev
        squares.append(jnp.sum(sq, axis=1, keepdims=True))
        bases.append(base)
    lane = lax.broadcasted_iota(jnp.int32, acc.shape, 1)
    acc = jnp.where(lane == SQUARES, jnp.concatenate(squares, axis=0), acc)
    acc = jnp.where(lane == VSUM, jnp.concatenate(bases, axis=0), acc)
    flat = jnp.transpose(acc)[0:ROWS, :]
    mean = flat[MEAN : MEAN + 1] / samples
    apart = mean - flat[VSUM : VSUM + 1]
    spread = jnp.maximum(flat[SQUARES : SQUARES + 1] - samples * apart * apart, 0.0)
    row = lax.broadcasted_iota(jnp.int32, flat.shape, 0)
    total = jnp.concatenate([vsum[0:1, :]] * (STEP // 128), axis=1)
    flat = jnp.where(row == MEAN, mean, jnp.where(row == SQUARES, spread, flat))
    return jnp.where(row == VSUM, total, flat)


def first_kernel(place, probes, phenotype, genotype, held, other, vec, vsum, arrived):
    variants, samples = genotype.shape
    steps = variants // STEP
    ahead = steps // 2
    away = (1 - (place[0] // 4) % 2) * ahead

    def copy(i):
        source = pl.ds(pl.multiple_of(((i + away) % steps) * STEP, STEP), STEP)
        target = pl.ds(pl.multiple_of(i * STEP, STEP), STEP)
        return pltpu.make_async_copy(genotype.at[source], held.at[target], arrived.at[i])

    for i in range(ahead):
        copy(i).start()
    row = lax.broadcasted_iota(jnp.int32, (32, samples), 0)
    low = jnp.concatenate([probes[...].astype(jnp.float32), jnp.zeros((12, samples), jnp.float32)], axis=0)
    phen = phenotype[...].astype(jnp.float32).reshape(1, samples)
    low = jnp.where(row == NV - 1, phen, jnp.where(row == MEAN, 1.0, low))
    full = jnp.concatenate([low, jnp.zeros((96, samples), jnp.float32)], axis=0)
    vec[...] = jnp.transpose(full).astype(jnp.bfloat16)
    vsum[...] = jnp.dot(jnp.ones((8, samples), jnp.bfloat16), vec[...], preferred_element_type=jnp.float32)

    def step(i, carry):
        copy(i).wait()
        copy(i + ahead).start()
        other[:, pl.ds(pl.multiple_of(i * STEP, STEP), STEP)] = block_stats(held, i * STEP, vec, vsum)
        return carry

    lax.fori_loop(0, ahead, step, 0)
    for i in range(ahead, steps):
        copy(i).wait()


def second_kernel(held, vec, vsum, mine):
    half = held.shape[0] // 2

    def step(i, carry):
        mine[:, pl.ds(pl.multiple_of(i * STEP, STEP), STEP)] = block_stats(held, half + i * STEP, vec, vsum)
        return carry

    lax.fori_loop(0, half // STEP, step, 0)


def local_stats(place, probes, phenotype, genotype):
    variants, samples = genotype.shape
    vmem = pl.BlockSpec(memory_space=pltpu.VMEM)
    block = jax.ShapeDtypeStruct((ROWS, variants // 2), jnp.float32)
    held, other, vec, vsum = pl.pallas_call(
        first_kernel,
        in_specs=[pl.BlockSpec(memory_space=pltpu.SMEM), vmem, vmem, pl.BlockSpec(memory_space=pltpu.HBM)],
        out_specs=(vmem, vmem, vmem, vmem),
        out_shape=(
            jax.ShapeDtypeStruct(genotype.shape, genotype.dtype),
            block,
            jax.ShapeDtypeStruct((samples, 128), jnp.bfloat16),
            jax.ShapeDtypeStruct((8, 128), jnp.float32),
        ),
        scratch_shapes=[pltpu.SemaphoreType.DMA((variants // STEP,))],
        compiler_params=pltpu.CompilerParams(vmem_limit_bytes=40 * 1024 * 1024),
        name="first_stats",
    )(place, probes, phenotype, genotype)
    theirs = shifted(other, "smp", ZLO_SWAP)
    mine = pl.pallas_call(
        second_kernel,
        in_specs=[vmem, vmem, vmem],
        out_specs=vmem,
        out_shape=block,
        compiler_params=pltpu.CompilerParams(vmem_limit_bytes=16 * 1024 * 1024),
        name="second_stats",
    )(held, vec, vsum)
    return held, mine, theirs


def merged(pieces, each):
    total = sum(pieces[1:], pieces[0])
    mean = total[MEAN : MEAN + 1] * (1.0 / len(pieces))
    apart = sum((p[MEAN : MEAN + 1] - mean) ** 2 for p in pieces) * each
    row = lax.broadcasted_iota(jnp.int32, total.shape, 0)
    return jnp.where(row == MEAN, mean, jnp.where(row == SQUARES, total + apart, total))


def over_samples(mine, theirs, samples):
    own = merged([mine, theirs], samples)
    own = merged([own, shifted(own, "smp", X_SWAP)], 2 * samples)
    own = merged([own, shifted(own, "smp", X_TURN)], 4 * samples)
    return own, shifted(own, "smp", ZLO_SWAP)


PAIRS = NV // 2
PACK = 88


def weigh(stats, tags, weights, shift):
    mean = stats[MEAN : MEAN + 1]
    scale = lax.rsqrt(stats[SQUARES : SQUARES + 1] / N + EPS)
    sub = lax.broadcasted_iota(jnp.int32, (ROWS, 128), 0)
    lane = lax.broadcasted_iota(jnp.int32, (ROWS, 128), 1)
    vsum = jnp.sum(jnp.where(sub == lane, stats[VSUM : VSUM + 1, 0:128], 0.0), axis=1, keepdims=True)
    projected = (stats - vsum * mean) * scale
    weight = projected * scale
    member = lax.broadcasted_iota(jnp.int32, (K, stats.shape[1]), 0) == tags
    counts = jnp.sum(jnp.where(member, 1.0, 0.0), axis=1, keepdims=True)

    def rows_of(j):
        return jnp.where(member, weight[j : j + 1], 0.0)

    for pair in range(PAIRS + 1):
        first = rows_of(2 * pair)
        second = rows_of(2 * pair + 1) if pair < PAIRS else jnp.zeros_like(first)
        weights[16 * pair : 16 * pair + 16, :] = jnp.concatenate([first, second], axis=0).astype(jnp.bfloat16)
    for r in range(0, 2 * PACK, 16):
        rows = weights[r : r + 16, :].astype(jnp.float32)
        shift[r : r + 16, :] = jnp.broadcast_to(jnp.sum(rows * mean, axis=1, keepdims=True), (16, 128))
    shift[K * NV :, :] = jnp.broadcast_to(-counts, (K, 128))


def own_kernel(place, own, labels, held, part, weights, shift):
    samples = held.shape[1]
    half = own.shape[1]
    lower = (place[0] // 4) % 2 == 0
    weigh(own[...], jnp.where(lower, labels[:, :half], labels[:, half:]), weights, shift)
    for c in range(0, samples, 256):
        block = jnp.dot(weights[...], held[half:, c : c + 256], preferred_element_type=jnp.float32)
        for h in range(0, 256, 128):
            part[:, c + h : c + h + 128] = block[:, h : h + 128] - shift[...]


def terms_kernel(place, back, labels, held, part, keep, give, weights, shift):
    samples = held.shape[1]
    half = back.shape[1]
    lower = (place[0] // 4) % 2 == 0
    weigh(back[...], jnp.where(lower, labels[:, half:], labels[:, :half]), weights, shift)
    spot = place[0] // 8
    y, z, core = spot // 8, (spot // 2) % 4, spot % 2
    low_lanes = lax.broadcasted_iota(jnp.int32, (PACK, 128), 1) < 64
    for c in range(samples // 256):
        block = jnp.dot(weights[...], held[:half, 256 * c : 256 * c + 256], preferred_element_type=jnp.float32)
        for h in range(2):
            t = 2 * c + h
            tile = block[:, 128 * h : 128 * h + 128] + (part[:, 128 * t : 128 * t + 128] - shift[...])
            a, b = tile[:PACK], tile[PACK:]
            ra, rb = pltpu.roll(a, 64, 1), pltpu.roll(b, 64, 1)
            zero = jnp.where(low_lanes, a, rb)
            one = jnp.where(low_lanes, ra, b)
            ky, kz = (t // 4 - y + 4) % 4, (t % 4 - z + 4) % 4
            keep[ky, kz] = jnp.where(core == 0, zero, one)
            give[ky, kz] = jnp.where(core == 0, one, zero)


def local_terms(place, own, back, labels, held):
    vmem = pl.BlockSpec(memory_space=pltpu.VMEM)
    smem = pl.BlockSpec(memory_space=pltpu.SMEM)
    samples = held.shape[1]
    tiles = jax.ShapeDtypeStruct((4, 4, PACK, 128), jnp.float32)
    scratch = [pltpu.VMEM((2 * PACK, own.shape[1]), jnp.bfloat16), pltpu.VMEM((2 * PACK, 128), jnp.float32)]
    params = pltpu.CompilerParams(vmem_limit_bytes=16 * 1024 * 1024)
    part = pl.pallas_call(
        own_kernel,
        in_specs=[smem, vmem, vmem, vmem],
        out_specs=vmem,
        out_shape=jax.ShapeDtypeStruct((2 * PACK, samples), jnp.float32),
        scratch_shapes=scratch,
        compiler_params=params,
        name="own_terms",
    )(place, own, labels, held)
    return pl.pallas_call(
        terms_kernel,
        in_specs=[smem, vmem, vmem, vmem, vmem],
        out_specs=(vmem, vmem),
        out_shape=(tiles, tiles),
        scratch_shapes=scratch,
        compiler_params=params,
        name="local_terms",
    )(place, back, labels, held, part)


def direct_sum(parts, axis, up, across, down):
    here, above, far, below = parts
    return here + shifted(above, axis, up) + shifted(below, axis, down) + shifted(far, axis, across)


def over_variants(keep, give):
    whole = keep + shifted(give, "var", CORE_SWAP)
    column = direct_sum([whole[k] for k in range(4)], "var", Y_UP, Y_ACROSS, Y_DOWN)
    return direct_sum([column[k] for k in range(4)], "var", Z_UP, Z_ACROSS, Z_DOWN)


def body(genotype, labels, probes, phenotype):
    variants, samples = genotype.shape
    place = lax.axis_index(("var", "smp")).astype(jnp.int32).reshape(1)
    held, mine, theirs = local_stats(place, probes, phenotype, genotype)
    own, back = over_samples(mine, theirs, samples)
    keep, give = local_terms(place, own, back, labels.reshape(1, variants), held)
    packed = over_variants(keep, give)
    rows = jnp.concatenate([packed[:, :64], packed[:, 64:]], axis=0).reshape(NV + 1, K, 64)
    out = rows[:NV] / rows[NV:]
    return jnp.transpose(out, (1, 0, 2)).reshape(K, NV, 1, 64)


def solution(mesh):
    placed = (P("var", "smp"), P("var"), P(None, "smp"), P("smp"))
    return jax.shard_map(
        body, mesh=mesh, in_specs=placed, out_specs=P(None, None, "smp", "var"), check_vma=False
    )
```

```python
import jax
import jax.numpy as jnp
from jax import lax
from jax.experimental import pallas as pl
from jax.experimental.pallas import tpu as pltpu
from jax.sharding import PartitionSpec as P

K = 8
NV = 21
EPS = 1e-06
N = 16384

MEAN, SQUARES, VSUM = 21, 22, 23
ROWS = 24
STEP = 256


def shifted(array, axis, perm):
    return lax.ppermute(array, axis, perm)


ZLO_SWAP = [(i, i ^ 4) for i in range(8)]
X_SWAP = [(i, i ^ 1) for i in range(8)]
X_TURN = [(i, i ^ 3) for i in range(8)]
CORE_SWAP = [(i, i ^ 1) for i in range(32)]
Y_UP = [(i, (i + 8) % 32) for i in range(32)]
Y_ACROSS = [(i, (i + 16) % 32) for i in range(32)]
Y_DOWN = [(i, (i - 8) % 32) for i in range(32)]
Z_UP = [(i, (i & 25) | ((i + 2) & 6)) for i in range(32)]
Z_ACROSS = [(i, i ^ 4) for i in range(32)]
Z_DOWN = [(i, (i & 25) | ((i - 2) & 6)) for i in range(32)]


def block_side(held, first):
    samples = held.shape[1]
    lane = lax.broadcasted_iota(jnp.int32, (64, 128), 1)
    sides = []
    for r in range(0, STEP, 64):
        part = pl.ds(pl.multiple_of(first + r, 64), 64)
        base = jnp.broadcast_to(held[part, 0:128].astype(jnp.float32)[:, 0:1], (64, 128))
        sq = jnp.zeros((64, 128), jnp.float32)
        for c in range(0, samples, 128):
            dev = held[part, c : c + 128].astype(jnp.float32) - base
            sq = sq + dev * dev
        sides.append(jnp.where(lane == SQUARES, jnp.sum(sq, axis=1, keepdims=True), base))
    return jnp.concatenate(sides, axis=0)


def block_stats(held, first, side, vec, vsum):
    samples = held.shape[1]
    rows = pl.ds(pl.multiple_of(first, STEP), STEP)
    acc = jnp.dot(held[rows, :], vec[...], preferred_element_type=jnp.float32)
    lane = lax.broadcasted_iota(jnp.int32, acc.shape, 1)
    flat = jnp.transpose(jnp.where(lane >= SQUARES, side, acc))[0:ROWS, :]
    mean = flat[MEAN : MEAN + 1] / samples
    apart = mean - flat[VSUM : VSUM + 1]
    spread = jnp.maximum(flat[SQUARES : SQUARES + 1] - samples * apart * apart, 0.0)
    row = lax.broadcasted_iota(jnp.int32, flat.shape, 0)
    total = jnp.concatenate([vsum[0:1, :]] * (STEP // 128), axis=1)
    flat = jnp.where(row == MEAN, mean, jnp.where(row == SQUARES, spread, flat))
    return jnp.where(row == VSUM, total, flat)


def hold_kernel(place, genotype, held, side, arrived):
    variants, samples = genotype.shape
    steps = variants // STEP
    ahead = steps // 2
    away = (1 - (place[0] // 4) % 2) * ahead

    def copy(i):
        source = pl.ds(pl.multiple_of(((i + away) % steps) * STEP, STEP), STEP)
        target = pl.ds(pl.multiple_of(i * STEP, STEP), STEP)
        return pltpu.make_async_copy(genotype.at[source], held.at[target], arrived.at[i])

    for i in range(ahead):
        copy(i).start()

    def step(i, carry):
        copy(i).wait()
        copy(i + ahead).start()
        side[pl.ds(pl.multiple_of(i * STEP, STEP), STEP), :] = block_side(held, i * STEP)
        return carry

    lax.fori_loop(0, ahead, step, 0)
    for i in range(ahead, steps):
        copy(i).wait()


def first_kernel(held, side, probes, phenotype, other, vec, vsum):
    samples = held.shape[1]
    half = held.shape[0] // 2
    row = lax.broadcasted_iota(jnp.int32, (32, samples), 0)
    low = jnp.concatenate([probes[...].astype(jnp.float32), jnp.zeros((12, samples), jnp.float32)], axis=0)
    phen = phenotype[...].astype(jnp.float32).reshape(1, samples)
    low = jnp.where(row == NV - 1, phen, jnp.where(row == MEAN, 1.0, low))
    full = jnp.concatenate([low, jnp.zeros((96, samples), jnp.float32)], axis=0)
    vec[...] = jnp.transpose(full).astype(jnp.bfloat16)
    vsum[...] = jnp.dot(jnp.ones((8, samples), jnp.bfloat16), vec[...], preferred_element_type=jnp.float32)

    def step(i, carry):
        rows = pl.ds(pl.multiple_of(i * STEP, STEP), STEP)
        other[:, rows] = block_stats(held, i * STEP, side[rows, :], vec, vsum)
        return carry

    lax.fori_loop(0, half // STEP, step, 0)


def second_kernel(held, vec, vsum, mine):
    half = held.shape[0] // 2

    def step(i, carry):
        rows = pl.ds(pl.multiple_of(i * STEP, STEP), STEP)
        first = half + i * STEP
        mine[:, rows] = block_stats(held, first, block_side(held, first), vec, vsum)
        return carry

    lax.fori_loop(0, half // STEP, step, 0)


def local_stats(place, probes, phenotype, genotype):
    variants, samples = genotype.shape
    vmem = pl.BlockSpec(memory_space=pltpu.VMEM)
    block = jax.ShapeDtypeStruct((ROWS, variants // 2), jnp.float32)
    small = pltpu.CompilerParams(vmem_limit_bytes=16 * 1024 * 1024)
    held, side = pl.pallas_call(
        hold_kernel,
        in_specs=[pl.BlockSpec(memory_space=pltpu.SMEM), pl.BlockSpec(memory_space=pltpu.HBM)],
        out_specs=(vmem, vmem),
        out_shape=(
            jax.ShapeDtypeStruct(genotype.shape, genotype.dtype),
            jax.ShapeDtypeStruct((variants // 2, 128), jnp.float32),
        ),
        scratch_shapes=[pltpu.SemaphoreType.DMA((variants // STEP,))],
        compiler_params=pltpu.CompilerParams(vmem_limit_bytes=40 * 1024 * 1024),
        cost_estimate=pl.CostEstimate(flops=40_000_000, bytes_accessed=2 * variants * samples, transcendentals=0),
        name="hold_genotype",
    )(place, genotype)
    other, vec, vsum = pl.pallas_call(
        first_kernel,
        in_specs=[vmem, vmem, vmem, vmem],
        out_specs=(vmem, vmem, vmem),
        out_shape=(
            block,
            jax.ShapeDtypeStruct((samples, 128), jnp.bfloat16),
            jax.ShapeDtypeStruct((8, 128), jnp.float32),
        ),
        compiler_params=small,
        name="first_stats",
    )(held, side, probes, phenotype)
    theirs = shifted(other, "smp", ZLO_SWAP)
    mine = pl.pallas_call(
        second_kernel,
        in_specs=[vmem, vmem, vmem],
        out_specs=vmem,
        out_shape=block,
        compiler_params=small,
        name="second_stats",
    )(held, vec, vsum)
    return held, mine, theirs


def merged(pieces, each):
    total = sum(pieces[1:], pieces[0])
    mean = total[MEAN : MEAN + 1] * (1.0 / len(pieces))
    apart = sum((p[MEAN : MEAN + 1] - mean) ** 2 for p in pieces) * each
    row = lax.broadcasted_iota(jnp.int32, total.shape, 0)
    return jnp.where(row == MEAN, mean, jnp.where(row == SQUARES, total + apart, total))


def over_samples(mine, theirs, samples):
    own = merged([mine, theirs], samples)
    own = merged([own, shifted(own, "smp", X_SWAP)], 2 * samples)
    own = merged([own, shifted(own, "smp", X_TURN)], 4 * samples)
    return own, shifted(own, "smp", ZLO_SWAP)


PAIRS = NV // 2
PACK = 88


def weigh(stats, tags, weights, shift):
    mean = stats[MEAN : MEAN + 1]
    scale = lax.rsqrt(stats[SQUARES : SQUARES + 1] / N + EPS)
    sub = lax.broadcasted_iota(jnp.int32, (ROWS, 128), 0)
    lane = lax.broadcasted_iota(jnp.int32, (ROWS, 128), 1)
    vsum = jnp.sum(jnp.where(sub == lane, stats[VSUM : VSUM + 1, 0:128], 0.0), axis=1, keepdims=True)
    projected = (stats - vsum * mean) * scale
    weight = projected * scale
    member = lax.broadcasted_iota(jnp.int32, (K, stats.shape[1]), 0) == tags
    counts = jnp.sum(jnp.where(member, 1.0, 0.0), axis=1, keepdims=True)

    def rows_of(j):
        return jnp.where(member, weight[j : j + 1], 0.0)

    for pair in range(PAIRS + 1):
        first = rows_of(2 * pair)
        second = rows_of(2 * pair + 1) if pair < PAIRS else jnp.zeros_like(first)
        weights[16 * pair : 16 * pair + 16, :] = jnp.concatenate([first, second], axis=0).astype(jnp.bfloat16)
    for r in range(0, 2 * PACK, 16):
        rows = weights[r : r + 16, :].astype(jnp.float32)
        shift[r : r + 16, :] = jnp.broadcast_to(jnp.sum(rows * mean, axis=1, keepdims=True), (16, 128))
    shift[K * NV :, :] = jnp.broadcast_to(-counts, (K, 128))


def own_kernel(place, own, labels, held, part, weights, shift):
    samples = held.shape[1]
    half = own.shape[1]
    lower = (place[0] // 4) % 2 == 0
    weigh(own[...], jnp.where(lower, labels[:, :half], labels[:, half:]), weights, shift)
    for c in range(0, samples, 256):
        block = jnp.dot(weights[...], held[half:, c : c + 256], preferred_element_type=jnp.float32)
        for h in range(0, 256, 128):
            part[:, c + h : c + h + 128] = block[:, h : h + 128] - shift[...]


def terms_kernel(place, back, labels, held, part, keep, give, weights, shift):
    samples = held.shape[1]
    half = back.shape[1]
    lower = (place[0] // 4) % 2 == 0
    weigh(back[...], jnp.where(lower, labels[:, half:], labels[:, :half]), weights, shift)
    spot = place[0] // 8
    y, z, core = spot // 8, (spot // 2) % 4, spot % 2
    low_lanes = lax.broadcasted_iota(jnp.int32, (PACK, 128), 1) < 64
    for c in range(samples // 256):
        block = jnp.dot(weights[...], held[:half, 256 * c : 256 * c + 256], preferred_element_type=jnp.float32)
        for h in range(2):
            t = 2 * c + h
            tile = block[:, 128 * h : 128 * h + 128] + (part[:, 128 * t : 128 * t + 128] - shift[...])
            a, b = tile[:PACK], tile[PACK:]
            ra, rb = pltpu.roll(a, 64, 1), pltpu.roll(b, 64, 1)
            zero = jnp.where(low_lanes, a, rb)
            one = jnp.where(low_lanes, ra, b)
            ky, kz = (t // 4 - y + 4) % 4, (t % 4 - z + 4) % 4
            keep[ky, kz] = jnp.where(core == 0, zero, one)
            give[ky, kz] = jnp.where(core == 0, one, zero)


def local_terms(place, own, back, labels, held):
    vmem = pl.BlockSpec(memory_space=pltpu.VMEM)
    smem = pl.BlockSpec(memory_space=pltpu.SMEM)
    samples = held.shape[1]
    tiles = jax.ShapeDtypeStruct((4, 4, PACK, 128), jnp.float32)
    scratch = [pltpu.VMEM((2 * PACK, own.shape[1]), jnp.bfloat16), pltpu.VMEM((2 * PACK, 128), jnp.float32)]
    params = pltpu.CompilerParams(vmem_limit_bytes=16 * 1024 * 1024)
    part = pl.pallas_call(
        own_kernel,
        in_specs=[smem, vmem, vmem, vmem],
        out_specs=vmem,
        out_shape=jax.ShapeDtypeStruct((2 * PACK, samples), jnp.float32),
        scratch_shapes=scratch,
        compiler_params=params,
        name="own_terms",
    )(place, own, labels, held)
    return pl.pallas_call(
        terms_kernel,
        in_specs=[smem, vmem, vmem, vmem, vmem],
        out_specs=(vmem, vmem),
        out_shape=(tiles, tiles),
        scratch_shapes=scratch,
        compiler_params=params,
        name="local_terms",
    )(place, back, labels, held, part)


def direct_sum(parts, axis, up, across, down):
    here, above, far, below = parts
    return here + shifted(above, axis, up) + shifted(below, axis, down) + shifted(far, axis, across)


def over_variants(keep, give):
    whole = keep + shifted(give, "var", CORE_SWAP)
    column = direct_sum([whole[k] for k in range(4)], "var", Y_UP, Y_ACROSS, Y_DOWN)
    return direct_sum([column[k] for k in range(4)], "var", Z_UP, Z_ACROSS, Z_DOWN)


def body(genotype, labels, probes, phenotype):
    variants, samples = genotype.shape
    place = lax.axis_index(("var", "smp")).astype(jnp.int32).reshape(1)
    held, mine, theirs = local_stats(place, probes, phenotype, genotype)
    own, back = over_samples(mine, theirs, samples)
    keep, give = local_terms(place, own, back, labels.reshape(1, variants), held)
    packed = over_variants(keep, give)
    rows = jnp.concatenate([packed[:, :64], packed[:, 64:]], axis=0).reshape(NV + 1, K, 64)
    out = rows[:NV] / rows[NV:]
    return jnp.transpose(out, (1, 0, 2)).reshape(K, NV, 1, 64)


def solution(mesh):
    placed = (P("var", "smp"), P("var"), P(None, "smp"), P("smp"))
    return jax.shard_map(
        body, mesh=mesh, in_specs=placed, out_specs=P(None, None, "smp", "var"), check_vma=False
    )
```

```python
import jax
import jax.numpy as jnp
from jax import lax
from jax.experimental import pallas as pl
from jax.experimental.pallas import tpu as pltpu
from jax.sharding import PartitionSpec as P

K = 8
NV = 21
EPS = 1e-06
N = 16384

MEAN, SQUARES, VSUM = 21, 22, 23
ROWS = 24
STEP = 256


def shifted(array, axis, perm):
    return lax.ppermute(array, axis, perm)


ZLO_SWAP = [(i, i ^ 4) for i in range(8)]
X_SWAP = [(i, i ^ 1) for i in range(8)]
X_TURN = [(i, i ^ 3) for i in range(8)]
CORE_SWAP = [(i, i ^ 1) for i in range(32)]
Y_UP = [(i, (i + 8) % 32) for i in range(32)]
Y_ACROSS = [(i, (i + 16) % 32) for i in range(32)]
Y_DOWN = [(i, (i - 8) % 32) for i in range(32)]
Z_UP = [(i, (i & 25) | ((i + 2) & 6)) for i in range(32)]
Z_ACROSS = [(i, i ^ 4) for i in range(32)]
Z_DOWN = [(i, (i & 25) | ((i - 2) & 6)) for i in range(32)]


def block_side(held, first):
    samples = held.shape[1]
    lane = lax.broadcasted_iota(jnp.int32, (64, 128), 1)
    sides = []
    for r in range(0, STEP, 64):
        part = pl.ds(pl.multiple_of(first + r, 64), 64)
        base = jnp.broadcast_to(held[part, 0:128].astype(jnp.float32)[:, 0:1], (64, 128))
        sq = jnp.zeros((64, 128), jnp.float32)
        for c in range(0, samples, 128):
            dev = held[part, c : c + 128].astype(jnp.float32) - base
            sq = sq + dev * dev
        sides.append(jnp.where(lane == SQUARES, jnp.sum(sq, axis=1, keepdims=True), base))
    return jnp.concatenate(sides, axis=0)


def block_stats(held, first, side, vec, vsum):
    samples = held.shape[1]
    rows = pl.ds(pl.multiple_of(first, STEP), STEP)
    acc = jnp.dot(held[rows, :], vec[...], preferred_element_type=jnp.float32)
    lane = lax.broadcasted_iota(jnp.int32, acc.shape, 1)
    flat = jnp.transpose(jnp.where(lane >= SQUARES, side, acc))[0:ROWS, :]
    mean = flat[MEAN : MEAN + 1] / samples
    apart = mean - flat[VSUM : VSUM + 1]
    spread = jnp.maximum(flat[SQUARES : SQUARES + 1] - samples * apart * apart, 0.0)
    row = lax.broadcasted_iota(jnp.int32, flat.shape, 0)
    total = jnp.concatenate([vsum[0:1, :]] * (STEP // 128), axis=1)
    flat = jnp.where(row == MEAN, mean, jnp.where(row == SQUARES, spread, flat))
    return jnp.where(row == VSUM, total, flat)


def hold_kernel(place, genotype, held, side, arrived):
    variants, samples = genotype.shape
    steps = variants // STEP
    ahead = steps // 2
    away = (1 - (place[0] // 4) % 2) * ahead

    def copy(i):
        source = pl.ds(pl.multiple_of(((i + away) % steps) * STEP, STEP), STEP)
        target = pl.ds(pl.multiple_of(i * STEP, STEP), STEP)
        return pltpu.make_async_copy(genotype.at[source], held.at[target], arrived.at[i])

    for i in range(ahead):
        copy(i).start()

    copy(0).wait()
    for i in range(ahead, steps):
        copy(i).start()

    def step(i, carry):
        @pl.when(i > 0)
        def _():
            copy(i).wait()

        side[pl.ds(pl.multiple_of(i * STEP, STEP), STEP), :] = block_side(held, i * STEP)
        return carry

    lax.fori_loop(0, ahead, step, 0)
    for i in range(ahead, steps):
        copy(i).wait()


def first_kernel(held, side, probes, phenotype, other, vec, vsum):
    samples = held.shape[1]
    half = held.shape[0] // 2
    row = lax.broadcasted_iota(jnp.int32, (32, samples), 0)
    low = jnp.concatenate([probes[...].astype(jnp.float32), jnp.zeros((12, samples), jnp.float32)], axis=0)
    phen = phenotype[...].astype(jnp.float32).reshape(1, samples)
    low = jnp.where(row == NV - 1, phen, jnp.where(row == MEAN, 1.0, low))
    full = jnp.concatenate([low, jnp.zeros((96, samples), jnp.float32)], axis=0)
    vec[...] = jnp.transpose(full).astype(jnp.bfloat16)
    vsum[...] = jnp.dot(jnp.ones((8, samples), jnp.bfloat16), vec[...], preferred_element_type=jnp.float32)

    def step(i, carry):
        rows = pl.ds(pl.multiple_of(i * STEP, STEP), STEP)
        other[:, rows] = block_stats(held, i * STEP, side[rows, :], vec, vsum)
        return carry

    lax.fori_loop(0, half // STEP, step, 0)


def second_kernel(held, vec, vsum, mine):
    half = held.shape[0] // 2

    def step(i, carry):
        rows = pl.ds(pl.multiple_of(i * STEP, STEP), STEP)
        first = half + i * STEP
        mine[:, rows] = block_stats(held, first, block_side(held, first), vec, vsum)
        return carry

    lax.fori_loop(0, half // STEP, step, 0)


def local_stats(place, probes, phenotype, genotype):
    variants, samples = genotype.shape
    vmem = pl.BlockSpec(memory_space=pltpu.VMEM)
    block = jax.ShapeDtypeStruct((ROWS, variants // 2), jnp.float32)
    small = pltpu.CompilerParams(vmem_limit_bytes=16 * 1024 * 1024)
    held, side = pl.pallas_call(
        hold_kernel,
        in_specs=[pl.BlockSpec(memory_space=pltpu.SMEM), pl.BlockSpec(memory_space=pltpu.HBM)],
        out_specs=(vmem, vmem),
        out_shape=(
            jax.ShapeDtypeStruct(genotype.shape, genotype.dtype),
            jax.ShapeDtypeStruct((variants // 2, 128), jnp.float32),
        ),
        scratch_shapes=[pltpu.SemaphoreType.DMA((variants // STEP,))],
        compiler_params=pltpu.CompilerParams(vmem_limit_bytes=40 * 1024 * 1024),
        cost_estimate=pl.CostEstimate(flops=40_000_000, bytes_accessed=2 * variants * samples, transcendentals=0),
        name="hold_genotype",
    )(place, genotype)
    other, vec, vsum = pl.pallas_call(
        first_kernel,
        in_specs=[vmem, vmem, vmem, vmem],
        out_specs=(vmem, vmem, vmem),
        out_shape=(
            block,
            jax.ShapeDtypeStruct((samples, 128), jnp.bfloat16),
            jax.ShapeDtypeStruct((8, 128), jnp.float32),
        ),
        compiler_params=small,
        name="first_stats",
    )(held, side, probes, phenotype)
    theirs = shifted(other, "smp", ZLO_SWAP)
    mine = pl.pallas_call(
        second_kernel,
        in_specs=[vmem, vmem, vmem],
        out_specs=vmem,
        out_shape=block,
        compiler_params=small,
        name="second_stats",
    )(held, vec, vsum)
    return held, mine, theirs


def merged(pieces, each):
    total = sum(pieces[1:], pieces[0])
    mean = total[MEAN : MEAN + 1] * (1.0 / len(pieces))
    apart = sum((p[MEAN : MEAN + 1] - mean) ** 2 for p in pieces) * each
    row = lax.broadcasted_iota(jnp.int32, total.shape, 0)
    return jnp.where(row == MEAN, mean, jnp.where(row == SQUARES, total + apart, total))


def over_samples(mine, theirs, samples):
    own = merged([mine, theirs], samples)
    own = merged([own, shifted(own, "smp", X_SWAP)], 2 * samples)
    own = merged([own, shifted(own, "smp", X_TURN)], 4 * samples)
    return own, shifted(own, "smp", ZLO_SWAP)


PAIRS = NV // 2
PACK = 88


def weigh(stats, tags, weights, shift):
    mean = stats[MEAN : MEAN + 1]
    scale = lax.rsqrt(stats[SQUARES : SQUARES + 1] / N + EPS)
    sub = lax.broadcasted_iota(jnp.int32, (ROWS, 128), 0)
    lane = lax.broadcasted_iota(jnp.int32, (ROWS, 128), 1)
    vsum = jnp.sum(jnp.where(sub == lane, stats[VSUM : VSUM + 1, 0:128], 0.0), axis=1, keepdims=True)
    projected = (stats - vsum * mean) * scale
    weight = projected * scale
    member = lax.broadcasted_iota(jnp.int32, (K, stats.shape[1]), 0) == tags
    counts = jnp.sum(jnp.where(member, 1.0, 0.0), axis=1, keepdims=True)

    def rows_of(j):
        return jnp.where(member, weight[j : j + 1], 0.0)

    for pair in range(PAIRS + 1):
        first = rows_of(2 * pair)
        second = rows_of(2 * pair + 1) if pair < PAIRS else jnp.zeros_like(first)
        weights[16 * pair : 16 * pair + 16, :] = jnp.concatenate([first, second], axis=0).astype(jnp.bfloat16)
    for r in range(0, 2 * PACK, 16):
        rows = weights[r : r + 16, :].astype(jnp.float32)
        shift[r : r + 16, :] = jnp.broadcast_to(jnp.sum(rows * mean, axis=1, keepdims=True), (16, 128))
    shift[K * NV :, :] = jnp.broadcast_to(-counts, (K, 128))


def own_kernel(place, own, labels, held, part, weights, shift):
    samples = held.shape[1]
    half = own.shape[1]
    lower = (place[0] // 4) % 2 == 0
    weigh(own[...], jnp.where(lower, labels[:, :half], labels[:, half:]), weights, shift)
    for c in range(0, samples, 256):
        block = jnp.dot(weights[...], held[half:, c : c + 256], preferred_element_type=jnp.float32)
        for h in range(0, 256, 128):
            part[:, c + h : c + h + 128] = block[:, h : h + 128] - shift[...]


def terms_kernel(place, back, labels, held, part, keep, give, weights, shift):
    samples = held.shape[1]
    half = back.shape[1]
    lower = (place[0] // 4) % 2 == 0
    weigh(back[...], jnp.where(lower, labels[:, half:], labels[:, :half]), weights, shift)
    spot = place[0] // 8
    y, z, core = spot // 8, (spot // 2) % 4, spot % 2
    low_lanes = lax.broadcasted_iota(jnp.int32, (PACK, 128), 1) < 64
    for c in range(samples // 256):
        block = jnp.dot(weights[...], held[:half, 256 * c : 256 * c + 256], preferred_element_type=jnp.float32)
        for h in range(2):
            t = 2 * c + h
            tile = block[:, 128 * h : 128 * h + 128] + (part[:, 128 * t : 128 * t + 128] - shift[...])
            a, b = tile[:PACK], tile[PACK:]
            ra, rb = pltpu.roll(a, 64, 1), pltpu.roll(b, 64, 1)
            zero = jnp.where(low_lanes, a, rb)
            one = jnp.where(low_lanes, ra, b)
            ky, kz = (t // 4 - y + 4) % 4, (t % 4 - z + 4) % 4
            keep[ky, kz] = jnp.where(core == 0, zero, one)
            give[ky, kz] = jnp.where(core == 0, one, zero)


def local_terms(place, own, back, labels, held):
    vmem = pl.BlockSpec(memory_space=pltpu.VMEM)
    smem = pl.BlockSpec(memory_space=pltpu.SMEM)
    samples = held.shape[1]
    tiles = jax.ShapeDtypeStruct((4, 4, PACK, 128), jnp.float32)
    scratch = [pltpu.VMEM((2 * PACK, own.shape[1]), jnp.bfloat16), pltpu.VMEM((2 * PACK, 128), jnp.float32)]
    params = pltpu.CompilerParams(vmem_limit_bytes=16 * 1024 * 1024)
    part = pl.pallas_call(
        own_kernel,
        in_specs=[smem, vmem, vmem, vmem],
        out_specs=vmem,
        out_shape=jax.ShapeDtypeStruct((2 * PACK, samples), jnp.float32),
        scratch_shapes=scratch,
        compiler_params=params,
        name="own_terms",
    )(place, own, labels, held)
    return pl.pallas_call(
        terms_kernel,
        in_specs=[smem, vmem, vmem, vmem, vmem],
        out_specs=(vmem, vmem),
        out_shape=(tiles, tiles),
        scratch_shapes=scratch,
        compiler_params=params,
        name="local_terms",
    )(place, back, labels, held, part)


def direct_sum(parts, axis, up, across, down):
    here, above, far, below = parts
    return here + shifted(above, axis, up) + shifted(below, axis, down) + shifted(far, axis, across)


def over_variants(keep, give):
    whole = keep + shifted(give, "var", CORE_SWAP)
    column = direct_sum([whole[k] for k in range(4)], "var", Y_UP, Y_ACROSS, Y_DOWN)
    return direct_sum([column[k] for k in range(4)], "var", Z_UP, Z_ACROSS, Z_DOWN)


def body(genotype, labels, probes, phenotype):
    variants, samples = genotype.shape
    place = lax.axis_index(("var", "smp")).astype(jnp.int32).reshape(1)
    held, mine, theirs = local_stats(place, probes, phenotype, genotype)
    own, back = over_samples(mine, theirs, samples)
    keep, give = local_terms(place, own, back, labels.reshape(1, variants), held)
    packed = over_variants(keep, give)
    rows = jnp.concatenate([packed[:, :64], packed[:, 64:]], axis=0).reshape(NV + 1, K, 64)
    out = rows[:NV] / rows[NV:]
    return jnp.transpose(out, (1, 0, 2)).reshape(K, NV, 1, 64)


def solution(mesh):
    placed = (P("var", "smp"), P("var"), P(None, "smp"), P("smp"))
    return jax.shard_map(
        body, mesh=mesh, in_specs=placed, out_specs=P(None, None, "smp", "var"), check_vma=False
    )
```
